32 devices in a mesh: dp: 8 (over z, x), mp: 4 (over y, core).
Axes of the slice: x: 2, y: 2, z: 4, core: 2. Of those that a mesh axis runs over, the one named last changes fastest.
Arguments:
- hidden_in: bfloat16 [2, 1024, 3584], P(None, 'dp', 'mp'), may hold values from -6 to 6
- out_grad: bfloat16 [2, 1024, 3584], P(None, 'dp', 'mp'), may hold values from -1536 to 1536
- pack_fill: int32 [2, 8], P(None, 'dp'), may hold values from 1 to 128, as said below
- norm_gain: float32 [3584], P('mp'), may hold values from 0.5 to 1.5
- up_weight: bfloat16 [3584, 7168], P(None, 'mp'), may hold values from -0.09375 to 0.09375
- down_weight: bfloat16 [7168, 3584], P('mp'), may hold values from -0.0625 to 0.0625
Outputs:
- in_grad: bfloat16 [2, 1024, 3584], P(None, 'dp', 'mp')
- up_grad: float32 [3584, 7168], P('dp', 'mp')
- down_grad: float32 [7168, 3584], P('mp', 'dp')
- gain_grad: float32 [3584], P('mp')
The draws below stay inside these ranges and needn't reach their ends.
Inputs may be any that keep to these rules, and one draw needn't show every extreme that they name: pack_fill[m, p] real tokens stand at the start of pack p of microbatch m (positions p * 128 onward); the other positions of the pack are padding and carry no loss. In every draw the last pack of the first microbatch is full.
All inputs are finite; a program needn't handle non-finite values.
Results may differ from the reference program's by a relative error of at most 0.014.
Values may be sent and summed in bfloat16 or wider, within the bound.
A program may use at most 128 MiB of HBM per device.

```python
import jax
import jax.numpy as jnp
from jax import lax

D = 3584
FFW = 7168
TOK_DEV = 128
MICRO = 2
TOKENS = 1024
N_MP = 4


def draw_pack_fill(key, part):
    pack_count = TOKENS // TOK_DEV
    pack_pos = jnp.arange(pack_count, dtype=jnp.int32)
    fill_top = TOK_DEV // 16 + 15 * TOK_DEV // 16 * pack_pos * pack_pos // ((pack_count - 1) * (pack_count - 1))
    fill_low = fill_top // 2 + 1
    drawn = jax.random.randint(key, (MICRO, pack_count), fill_low[None, :], fill_top[None, :] + 1, dtype=jnp.int32)
    return drawn.at[0, pack_count - 1].set(TOK_DEV)


def block_scale(stream_key, shape, split, low, top_value):
    def one(dim, shards_of):
        heights = jax.random.uniform(jax.random.fold_in(jax.random.fold_in(stream_key, 6), dim), (shards_of,), jnp.float32, low / len(split), top_value / len(split))
        return jnp.repeat(jnp.exp(heights), shape[dim] // shards_of).reshape((-1,) + (1,) * (len(shape) - dim - 1))

    gain = one(*split[0])
    for cut in split[1:]:
        gain = gain * one(*cut)
    return gain


def normal_values(rng, shape, deviation, most, split=(), kind=jnp.bfloat16):
    loudness = block_scale(rng, shape, split, -0.22, 0.18) if split else 1.0
    entries = jax.random.normal(rng, shape, jnp.float32) * deviation * loudness
    return jnp.minimum(jnp.maximum(entries, -most), most).astype(kind)


def setup_inputs(seed: int = 0) -> dict:
    keys = jax.random.split(jax.random.key(seed), 7)
    hidden_in = normal_values(keys[0], (MICRO, TOKENS, D), 1.0, 6.0, ((1, 8), (2, 4)))
    out_grad = normal_values(keys[1], (MICRO, TOKENS, D), (MICRO * TOKENS // 8), 1536.0, ((1, 8), (2, 4)))
    pack_fill = draw_pack_fill(jax.random.fold_in(keys[6], 71), 0)
    norm_gain = jnp.clip(1.0 + 0.1 * jax.random.normal(keys[3], (D,), jnp.float32), 0.5, 1.5)
    up_weight = normal_values(keys[4], (D, FFW), D ** -0.5, 0.09375, ((1, 4),))
    down_weight = normal_values(keys[5], (FFW, D), FFW ** -0.5, 0.0625, ((0, 4),))
    return {"hidden_in": hidden_in, "out_grad": out_grad, "pack_fill": pack_fill, "norm_gain": norm_gain, "up_weight": up_weight, "down_weight": down_weight}


epsilon = 1e-06

def gelu_tanh(value):
    return jax.nn.gelu(value, approximate=True)

def contract_rows(left, right):
    return lax.dot_general(left, right, (((0,), (0,)), ((), ())), preferred_element_type=jnp.float32)

def contract_cols(left, right):
    return lax.dot_general(left, right, (((1,), (1,)), ((), ())), preferred_element_type=jnp.float32)

def group_sums(grad_pre, up_weight):
    row_count = grad_pre.shape[0]
    model_width = up_weight.shape[0]
    group_width = up_weight.shape[1] // N_MP
    pre_groups = grad_pre.reshape(row_count, N_MP, group_width).transpose(1, 0, 2)
    weight_groups = up_weight.reshape(model_width, N_MP, group_width).transpose(1, 0, 2)

    def add_group(total, pair):
        rounded = contract_cols(pair[0], pair[1]).astype(jnp.bfloat16)
        rounded = lax.optimization_barrier(rounded)
        return (total + rounded.astype(jnp.float32), None)
    total, unused = lax.scan(add_group, jnp.zeros((row_count, model_width), jnp.float32), (pre_groups, weight_groups))
    return total

def micro_grads(hidden_rows, grad_rows, live_mask, inv_count, norm_gain, up_weight, down_weight):
    model_width = hidden_rows.shape[1]
    values = hidden_rows.astype(jnp.float32)
    inv_rms = lax.rsqrt(lax.optimization_barrier(jnp.sum(values * values, axis=1, keepdims=True)) / model_width + epsilon)
    normed = (values * inv_rms * norm_gain[None, :]).astype(jnp.bfloat16)
    pre_act = jnp.dot(normed, up_weight, preferred_element_type=jnp.float32)
    activated = gelu_tanh(pre_act).astype(jnp.bfloat16)
    scaled = (grad_rows.astype(jnp.float32) * live_mask[:, None] * inv_count).astype(jnp.bfloat16)
    grad_act = contract_cols(scaled, down_weight)
    grad_pre = jax.vjp(gelu_tanh, pre_act)[1](grad_act)[0].astype(jnp.bfloat16)
    grad_normed = group_sums(grad_pre, up_weight)
    row_dot = lax.optimization_barrier(jnp.sum(grad_normed * norm_gain[None, :] * values, axis=1, keepdims=True))
    cubed = inv_rms * inv_rms * inv_rms
    in_rows = scaled.astype(jnp.float32) + norm_gain[None, :] * grad_normed * inv_rms - values * cubed * row_dot / model_width
    gain_term = lax.optimization_barrier(jnp.sum(grad_normed * values * inv_rms, axis=0))
    return (in_rows.astype(jnp.bfloat16), contract_rows(normed, grad_pre), contract_rows(activated, scaled), gain_term)

def reference(hidden_in, out_grad, pack_fill, norm_gain, up_weight, down_weight):
    token_total = jnp.sum(pack_fill).astype(jnp.float32)
    inv_count = 1.0 / token_total
    position = jnp.arange(TOKENS, dtype=jnp.int32)
    pack_index = position // TOK_DEV
    offset = position % TOK_DEV
    up_grad = jnp.zeros(up_weight.shape, jnp.float32)
    down_grad = jnp.zeros(down_weight.shape, jnp.float32)
    gain_grad = jnp.zeros(norm_gain.shape, jnp.float32)
    in_parts = []
    for micro_index in range(MICRO):
        live_mask = (offset < pack_fill[micro_index][pack_index]).astype(jnp.float32)
        in_rows, up_term, down_term, gain_term = micro_grads(hidden_in[micro_index], out_grad[micro_index], live_mask, inv_count, norm_gain, up_weight, down_weight)
        up_grad = up_grad + up_term
        down_grad = down_grad + down_term
        gain_grad = gain_grad + gain_term
        in_parts.append(in_rows)
    return (jnp.stack(in_parts), up_grad, down_grad, gain_grad)
```

```python
import functools

import jax
import jax.numpy as jnp
from jax import lax
from jax.experimental import pallas as pl
from jax.experimental.pallas import tpu as pltpu
from jax.sharding import PartitionSpec as P


epsilon = 1e-06


def gelu_tanh(value):
    return jax.nn.gelu(value, approximate=True)


def contract_rows(left, right):
    return lax.dot_general(
        left, right, (((0,), (0,)), ((), ())), preferred_element_type=jnp.float32
    )


def contract_cols(left, right):
    return lax.dot_general(
        left, right, (((1,), (1,)), ((), ())), preferred_element_type=jnp.float32
    )


def stripe(rows, n_dp):
    micro, tok, width = rows.shape
    parts = []
    for m in range(micro):
        part = rows[m].reshape(tok // n_dp, n_dp, width).transpose(1, 0, 2)
        parts.append(part[::-1] if m % 2 else part)
    return jnp.concatenate(parts, axis=1)


def unstripe(slots, micro):
    n_dp, per, width = slots.shape
    share = per // micro
    outs = []
    for m in range(micro):
        part = slots[:, m * share : (m + 1) * share]
        part = part[::-1] if m % 2 else part
        outs.append(part.transpose(1, 0, 2).reshape(share * n_dp, width))
    return jnp.stack(outs)


def flipped(index, bit):
    return index + bit - 2 * bit * lax.rem(lax.div(index, bit), 2)


def flipped_by(index, mask):
    bit = 1
    while bit <= mask:
        if mask & bit:
            index = flipped(index, bit)
        bit *= 2
    return index


def exchange_kernel(axes, *refs):
    count = len(axes)
    ins, outs = refs[:count], refs[count : 2 * count]
    sems = refs[2 * count :]
    barrier = pltpu.get_barrier_semaphore()
    greeted = 0
    for axis in sorted({axis for axis, _ in axes}):
        n, me = lax.axis_size(axis), lax.axis_index(axis)
        for d in range(1, n):
            pl.semaphore_signal(
                barrier,
                inc=1,
                device_id={axis: lax.rem(me + d, n)},
                device_id_type=pl.DeviceIdType.MESH,
            )
        greeted += n - 1
    pl.semaphore_wait(barrier, greeted)

    def send(k, axis, source, target, peer, slot):
        copy = pltpu.make_async_remote_copy(
            src_ref=source,
            dst_ref=outs[k].at[target],
            send_sem=sems[2 * k].at[slot],
            recv_sem=sems[2 * k + 1].at[slot],
            device_id={axis: peer},
            device_id_type=pl.DeviceIdType.MESH,
        )
        copy.start()
        return copy

    trees = [k for k, (_, kind) in enumerate(axes) if kind == "tree"]
    copies = {}

    def forward(k, mask, below):
        axis = axes[k][0]
        me = lax.axis_index(axis)
        owner = flipped_by(me, mask)
        bit = below
        while bit >= 1:
            copies[k, mask ^ bit] = send(
                k,
                axis,
                outs[k].at[owner] if mask else ins[k],
                owner,
                flipped(me, bit),
                mask ^ bit,
            )
            bit //= 2

    for k in trees:
        forward(k, 0, lax.axis_size(axes[k][0]) // 2)
    locals_ = []
    for k, (axis, kind) in enumerate(axes):
        n, me = lax.axis_size(axis), lax.axis_index(axis)
        for d in [n // 2] + [d for d in range(1, n) if d != n // 2]:
            if kind == "tree":
                break
            peer = lax.rem(me + d, n)
            source = ins[k].at[peer] if kind == "split" else ins[k]
            copies[k, d] = send(k, axis, source, me, peer, d)
        own = pltpu.make_async_copy(
            ins[k].at[me] if kind == "split" else ins[k],
            outs[k].at[me],
            sems[2 * k].at[0],
        )
        own.start()
        locals_.append(own)
    relayed = set()
    if trees:
        n = lax.axis_size(axes[trees[0]][0])
        for mask in sorted(range(2, n, 2), key=lambda m: (bin(m).count("1"), -m)):
            for k in trees:
                copies[k, mask].wait_recv()
                relayed.add((k, mask))
                forward(k, mask, (mask & -mask) // 2)
    for key, copy in copies.items():
        copy.wait_send()
        if key not in relayed:
            copy.wait_recv()
    for own in locals_:
        own.wait()


def exchange(arrays, axes, collective_id):
    shapes, sems = [], []
    for array, (axis, kind) in zip(arrays, axes):
        n = lax.axis_size(axis)
        block = array.shape[1:] if kind == "split" else array.shape
        shapes.append(jax.ShapeDtypeStruct((n,) + block, array.dtype))
        sems += [pltpu.SemaphoreType.DMA((n,)), pltpu.SemaphoreType.DMA((n,))]
    vmem = pl.BlockSpec(memory_space=pltpu.VMEM)
    return pl.pallas_call(
        functools.partial(exchange_kernel, axes),
        out_shape=shapes,
        in_specs=[vmem] * len(arrays),
        out_specs=[vmem] * len(arrays),
        scratch_shapes=sems,
        compiler_params=pltpu.CompilerParams(
            collective_id=collective_id, has_side_effects=True
        ),
    )(*arrays)


def on_device(hidden_in, out_grad, pack_fill, norm_gain, up_weight, down_weight):
    micro, tok, width = hidden_in.shape
    model_width, ff_shard = up_weight.shape
    n_dp, n_mp = lax.axis_size("dp"), lax.axis_size("mp")
    me = lax.axis_index("dp")
    share = tok // n_dp
    slot_count = n_dp * micro * share
    chunk = -(-slot_count * 3 // 8 // 16) * 16
    cols = model_width // n_dp

    sent = stripe(jnp.concatenate([hidden_in, out_grad], axis=2), n_dp)
    fill_tile = jnp.broadcast_to(pack_fill, (micro, 128))
    gain_tile = jnp.broadcast_to(norm_gain[None, :], (8, width))
    slots, fills, gain_full = exchange(
        [sent, fill_tile, gain_tile],
        (("dp", "split"), ("dp", "all"), ("mp", "all")),
        0,
    )
    slots = slots.reshape(slot_count, 2 * width)
    fills = fills[:, :, 0].T
    gain_full = gain_full[:, 0, :].reshape(model_width)
    inv_count = 1.0 / jnp.sum(fills).astype(jnp.float32)

    odd = (jnp.arange(micro, dtype=jnp.int32) % 2)[None, :, None]
    steps = jnp.arange(share, dtype=jnp.int32)[None, None, :]
    start = jnp.where(odd == 1, n_dp - 1 - me, me)
    live = (start + steps * n_dp < fills.T[:, :, None]).reshape(slot_count)
    slot_ids = jnp.arange(slot_count, dtype=jnp.int32)
    before = (slot_ids[None, :] < slot_ids[:, None]) & live[None, :]
    place = jnp.where(live, jnp.sum(before.astype(jnp.int32), axis=1), -1)

    ranks = jnp.arange(n_dp, dtype=jnp.int32)[:, None, None]
    starts = jnp.where(odd.reshape(1, micro, 1) == 1, n_dp - 1 - ranks, ranks)
    counts = jnp.clip((fills[None] - starts + n_dp - 1) // n_dp, 0, share)
    most = jnp.max(jnp.sum(counts, axis=(1, 2)))
    chunk_total = (most + chunk - 1) // chunk

    def run_chunk(index):
        spots = jnp.arange(chunk, dtype=jnp.int32) + index * chunk
        pick = (spots[:, None] == place[None, :]).astype(jnp.bfloat16)
        packed = jnp.dot(pick, slots, preferred_element_type=jnp.float32)
        tok_rows = packed[:, :width].astype(jnp.bfloat16)
        scaled = (packed[:, width:] * inv_count).astype(jnp.bfloat16)
        (both,) = exchange(
            [jnp.concatenate([tok_rows, scaled], axis=1)], (("mp", "all"),), 1
        )
        both = both.transpose(1, 0, 2)
        tok_full = both[:, :, :width].reshape(chunk, model_width).astype(jnp.float32)
        scaled_full = both[:, :, width:].reshape(chunk, model_width)
        squares = jnp.sum(tok_full * tok_full, axis=1, keepdims=True)
        inv_rms = lax.rsqrt(squares / model_width + epsilon)
        normed_full = (tok_full * inv_rms * gain_full[None, :]).astype(jnp.bfloat16)
        pre_act = jnp.dot(normed_full, up_weight, preferred_element_type=jnp.float32)
        activated = gelu_tanh(pre_act).astype(jnp.bfloat16)
        grad_act = contract_cols(scaled_full, down_weight)
        grad_pre = jax.vjp(gelu_tanh, pre_act)[1](grad_act)[0].astype(jnp.bfloat16)

        by_cols = jnp.concatenate(
            [
                normed_full.reshape(chunk, n_dp, cols),
                scaled_full.reshape(chunk, n_dp, cols),
            ],
            axis=2,
        ).transpose(1, 0, 2)

        row_part = jnp.sum(grad_pre.astype(jnp.float32) * pre_act, axis=1, keepdims=True)
        partial = contract_cols(grad_pre, up_weight).astype(jnp.bfloat16)
        shares, row_parts = exchange(
            [
                partial.reshape(chunk, n_mp, width).transpose(1, 0, 2),
                jnp.broadcast_to(row_part / inv_rms, (chunk, 128)),
            ],
            (("mp", "split"), ("mp", "all")),
            2,
        )
        grad_normed = jnp.sum(shares.astype(jnp.float32), axis=0)
        row_dot = jnp.sum(row_parts, axis=0)[:, :1]
        values = tok_rows.astype(jnp.float32)
        cubed = inv_rms * inv_rms * inv_rms
        in_rows = (
            scaled.astype(jnp.float32)
            + norm_gain[None, :] * grad_normed * inv_rms
            - values * cubed * row_dot / model_width
        ).astype(jnp.bfloat16)
        gain_term = jnp.sum(grad_normed * values * inv_rms, axis=0)
        back = contract_rows(pick, in_rows).astype(jnp.bfloat16)
        act_all, pre_all, by_cols, back, gain_parts = exchange(
            [
                activated,
                grad_pre,
                by_cols,
                back.reshape(n_dp, micro * share, width),
                jnp.broadcast_to(gain_term[None, :], (8, width)),
            ],
            (("dp", "tree"), ("dp", "tree"), ("dp", "split"), ("dp", "split"), ("dp", "all")),
            3,
        )
        by_cols = by_cols.reshape(n_dp * chunk, 2 * cols)
        up_term = contract_rows(by_cols[:, :cols], pre_all.reshape(n_dp * chunk, ff_shard))
        down_term = contract_rows(act_all.reshape(n_dp * chunk, ff_shard), by_cols[:, cols:])
        return (back, up_term, down_term, jnp.sum(gain_parts[:, 0], axis=0))

    def add_chunk(index, total):
        return jax.tree.map(jnp.add, total, run_chunk(index))

    total = run_chunk(jnp.int32(0))
    back, up_grad, down_grad, gain_acc = lax.fori_loop(1, chunk_total, add_chunk, total)
    return (unstripe(back, micro), up_grad, down_grad, gain_acc)


def solution(mesh):
    in_specs = (
        P(None, "dp", "mp"),
        P(None, "dp", "mp"),
        P(None, "dp"),
        P("mp"),
        P(None, "mp"),
        P("mp", None),
    )
    out_specs = (P(None, "dp", "mp"), P("dp", "mp"), P("mp", "dp"), P("mp"))
    return jax.shard_map(
        on_device, mesh=mesh, in_specs=in_specs, out_specs=out_specs, check_vma=False
    )
```
